128 devices in a mesh: freq: 64 (over y, x, z_lo, core), grid: 2 (over z_hi).
Axes of the slice: x: 4, y: 4, z: 4 (z_hi: 2, z_lo: 2; z = z_hi * 2 + z_lo), core: 2. Of those that a mesh axis runs over, the one named last changes fastest.
Arguments:
- cross_spectra: float32 [2, 128, 256, 256], P(None, None, 'freq', 'grid'), as said below
- sensor_modes: float32 [128, 96, 256], P('freq', None, 'grid'), may hold values from -0.375 to 0.375
- source_modes: float32 [128, 96, 256], P('freq', None, 'grid'), may hold values from -6 to 6
- wavenumber: float32 [128, 96], P('freq'), may hold values from 0.5 to 2
- attenuation: float32 [128, 96], P('freq'), may hold values from 0.002 to 0.03
- mode_counts: int32 [128], P('freq'), may hold values from 48 to 96
Outputs:
- bartlett_power: float32 [64, 256], P('freq', 'grid')
The draws below stay inside these ranges and needn't reach their ends.
Inputs may be any that keep to these rules, and one draw needn't show every extreme that they name: `cross_spectra`: each bin's matrix K_f is Hermitian and positive definite. Modes with index mode_counts[f] or more are left out in bin f.
All inputs are finite; a program needn't handle non-finite values.
Results may differ from the reference program's by a relative error of at most 0.0003.
Values sent between devices are 32-bit elements; how exact they have to be, the bound alone decides.
No kernel may reach another device: no remote copies, remote signals or barrier semaphores. Data moves between devices by JAX's collectives and lax.ppermute only.
A program may use at most 128 MiB of HBM per device.

```python
import math
import jax
import jax.numpy as jnp
from jax import lax

SENSORS = 256
MODES = 96
RANGES = 64
BINS = 128
DEPTHS = 256


def sensor_table(key):
    base = jax.random.fold_in(key, 201)
    values = jnp.clip(jax.random.normal(base, (BINS, MODES, SENSORS), jnp.float32), -6.0, 6.0)
    return (values / math.sqrt(SENSORS)).astype(jnp.float32)


def source_table(key):
    base = jax.random.fold_in(key, 202)
    values = jnp.clip(jax.random.normal(base, (BINS, MODES, DEPTHS), jnp.float32), -6.0, 6.0)
    return values.astype(jnp.float32)


def wave_table(key):
    base = jax.random.fold_in(key, 203)
    values = jnp.exp(jax.random.uniform(base, (BINS, MODES), jnp.float32, math.log(0.5), math.log(2.0)))
    return jnp.clip(values, 0.5, 2.0).astype(jnp.float32)


def atten_table(key):
    base = jax.random.fold_in(key, 204)
    values = jnp.exp(jax.random.uniform(base, (BINS, MODES), jnp.float32, math.log(0.002), math.log(0.03)))
    return jnp.clip(values, 0.002, 0.03).astype(jnp.float32)


def draw_sensor_modes(key, part):
    return sensor_table(key)


def draw_source_modes(key, part):
    return source_table(key)


def draw_wavenumber(key, part):
    return wave_table(key)


def draw_attenuation(key, part):
    return atten_table(key)


def draw_cross_spectra(key, part):
    snapshots = SENSORS // 2
    planted = 3
    key_real, key_imag, key_gain, key_bin, key_range, key_depth, key_power = jax.random.split(jax.random.fold_in(key, 17), 7)
    sample_real = jax.random.normal(key_real, (BINS, SENSORS, snapshots), jnp.float32) * math.sqrt(0.5)
    sample_imag = jax.random.normal(key_imag, (BINS, SENSORS, snapshots), jnp.float32) * math.sqrt(0.5)
    sensor_gain = jnp.exp(jax.random.uniform(key_gain, (BINS, SENSORS), jnp.float32, math.log(0.5), math.log(2.0)))
    bin_gain = jnp.exp(jax.random.uniform(key_bin, (BINS,), jnp.float32, math.log(0.3), math.log(3.0)))
    noise_real = (jnp.einsum('bis,bjs->bij', sample_real, sample_real) + jnp.einsum('bis,bjs->bij', sample_imag, sample_imag)) / snapshots
    noise_real = noise_real + jnp.eye(SENSORS, dtype=jnp.float32)[None]
    noise_imag = (jnp.einsum('bis,bjs->bij', sample_imag, sample_real) - jnp.einsum('bis,bjs->bij', sample_real, sample_imag)) / snapshots
    gain_outer = sensor_gain[:, :, None] * sensor_gain[:, None, :]
    noise_real = noise_real * gain_outer
    noise_imag = noise_imag * gain_outer
    shapes = sensor_table(key)
    sources = source_table(key)
    waves = wave_table(key)
    damping = atten_table(key)
    cell_range = jax.random.randint(key_range, (planted,), 0, RANGES)
    cell_depth = jax.random.randint(key_depth, (planted,), 0, DEPTHS)
    radius = 1.0 + cell_range.astype(jnp.float32)
    phase = waves[:, :, None] * radius[None, None, :]
    magnitude = jnp.exp(-damping[:, :, None] * radius[None, None, :]) / jnp.sqrt(phase)
    depth_shape = jnp.take(sources, cell_depth, axis=2)
    coef_real = magnitude * jnp.cos(phase) * depth_shape
    coef_imag = magnitude * jnp.sin(phase) * depth_shape
    steer_real = jnp.einsum('bmi,bmp->bpi', shapes, coef_real)
    steer_imag = jnp.einsum('bmi,bmp->bpi', shapes, coef_imag)
    length = jnp.sqrt(jnp.sum(steer_real * steer_real + steer_imag * steer_imag, axis=2, keepdims=True))
    unit_real = steer_real / length
    unit_imag = steer_imag / length
    noise_level = 2.0 * jnp.mean(sensor_gain * sensor_gain, axis=1)
    strength = jnp.exp(jax.random.uniform(key_power, (BINS, planted), jnp.float32, 0.0, math.log(10.0))) * noise_level[:, None]
    signal_real = jnp.einsum('bp,bpi,bpj->bij', strength, unit_real, unit_real) + jnp.einsum('bp,bpi,bpj->bij', strength, unit_imag, unit_imag)
    signal_imag = jnp.einsum('bp,bpi,bpj->bij', strength, unit_imag, unit_real) - jnp.einsum('bp,bpi,bpj->bij', strength, unit_real, unit_imag)
    real_part = (noise_real + signal_real) * bin_gain[:, None, None]
    imag_part = (noise_imag + signal_imag) * bin_gain[:, None, None]
    return jnp.stack([real_part, imag_part]).astype(jnp.float32)


def set_ends(result, stream_key, smallest, high):
    extent = result.shape
    index_at = [jax.random.randint(jax.random.fold_in(stream_key, axis), (), 0, extent[axis]) for axis in range(len(extent))]
    result = result.at[tuple(index_at)].set(smallest)
    longest = extent.index(max(extent))
    index_at[longest] = (index_at[longest] + 1) % extent[longest]
    return result.at[tuple(index_at)].set(high)


def setup_inputs(seed: int = 0) -> dict:
    keys = jax.random.split(jax.random.key(seed), 7)
    cross_spectra = draw_cross_spectra(jax.random.fold_in(keys[6], 71), 0)
    sensor_modes = draw_sensor_modes(jax.random.fold_in(keys[6], 71), 0)
    source_modes = draw_source_modes(jax.random.fold_in(keys[6], 71), 0)
    wavenumber = draw_wavenumber(jax.random.fold_in(keys[6], 71), 0)
    attenuation = draw_attenuation(jax.random.fold_in(keys[6], 71), 0)
    mode_counts = set_ends(jax.random.randint(keys[5], (BINS,), MODES // 2, MODES + 1), jax.random.fold_in(keys[5], 1), MODES // 2, MODES).astype(jnp.int32)
    return dict(cross_spectra=cross_spectra, sensor_modes=sensor_modes, source_modes=source_modes, wavenumber=wavenumber, attenuation=attenuation, mode_counts=mode_counts)


HIGH = lax.Precision.HIGHEST

def replica_terms(wave_row, atten_row, count, source_row, ranges):
    phase = wave_row[:, None] * ranges[None, :]
    magnitude = jnp.exp(-atten_row[:, None] * ranges[None, :]) / jnp.sqrt(phase)
    keep = (jnp.arange(source_row.shape[0], dtype=jnp.int32) < count).astype(jnp.float32)
    hankel_real = magnitude * jnp.cos(phase) * keep[:, None]
    hankel_imag = magnitude * jnp.sin(phase) * keep[:, None]
    coef_real = hankel_real[:, :, None] * source_row[:, None, :]
    coef_imag = hankel_imag[:, :, None] * source_row[:, None, :]
    return (coef_real, coef_imag)

def reference(cross_spectra, sensor_modes, source_modes, wavenumber, attenuation, mode_counts):
    ranges = 1.0 + jnp.arange(RANGES, dtype=jnp.float32)

    def one_bin(total, bin_index):
        spectra = cross_spectra[:, bin_index]
        shapes = sensor_modes[bin_index]
        product = jnp.einsum('cij,mj->cim', spectra, shapes, precision=HIGH)
        projected = jnp.einsum('mi,cin->cmn', shapes, product, precision=HIGH)
        gram = jnp.einsum('mi,ni->mn', shapes, shapes, precision=HIGH)
        coef_real, coef_imag = replica_terms(wavenumber[bin_index], attenuation[bin_index], mode_counts[bin_index], source_modes[bin_index], ranges)
        image_real = jnp.einsum('mn,nrz->mrz', projected[0], coef_real, precision=HIGH) - jnp.einsum('mn,nrz->mrz', projected[1], coef_imag, precision=HIGH)
        image_imag = jnp.einsum('mn,nrz->mrz', projected[1], coef_real, precision=HIGH) + jnp.einsum('mn,nrz->mrz', projected[0], coef_imag, precision=HIGH)
        numer = lax.optimization_barrier(jnp.sum(coef_real * image_real + coef_imag * image_imag, axis=0))
        gram_real = jnp.einsum('mn,nrz->mrz', gram, coef_real, precision=HIGH)
        gram_imag = jnp.einsum('mn,nrz->mrz', gram, coef_imag, precision=HIGH)
        denom = lax.optimization_barrier(jnp.sum(coef_real * gram_real + coef_imag * gram_imag, axis=0))
        return (total + numer / denom, None)
    total, unused = lax.scan(one_bin, jnp.zeros((RANGES, DEPTHS), jnp.float32), jnp.arange(BINS, dtype=jnp.int32))
    return total / BINS
```

```python
import jax
import jax.numpy as jnp
from jax import lax
from jax.experimental import pallas as pl
from jax.experimental.pallas import tpu as pltpu
from jax.sharding import PartitionSpec as P

RANGES = 64
LANES = 128
CHUNK = 8

VMEM = pl.BlockSpec(memory_space=pltpu.VMEM)
SMEM = pl.BlockSpec(memory_space=pltpu.SMEM)


def split(value):
    high = value.astype(jnp.bfloat16)
    low = (value - high.astype(jnp.float32)).astype(jnp.bfloat16)
    return high, low


def dot(left, right, contract=((1,), (0,))):
    return lax.dot_general(left, right, (contract, ((), ())), preferred_element_type=jnp.float32)


def pair_kernel(grid_ref, counts_ref, wave_ref, atten_ref, even_ref, odd_ref, row_real, row_imag, col_real, col_imag):
    modes = wave_ref.shape[1]
    mine = grid_ref[0]
    count = counts_ref[mine]
    ranges = 1.0 + lax.broadcasted_iota(jnp.int32, (RANGES, modes), 0).astype(jnp.float32)
    phase = wave_ref[pl.ds(mine, 1), :] * ranges
    magnitude = jnp.exp(-atten_ref[pl.ds(mine, 1), :] * ranges) / jnp.sqrt(phase)
    keep = lax.broadcasted_iota(jnp.int32, (RANGES, modes), 1) < count
    magnitude = jnp.where(keep, magnitude, 0.0)
    for row, col, value in (
        (row_real, col_real, magnitude * jnp.cos(phase)),
        (row_imag, col_imag, magnitude * jnp.sin(phase)),
    ):
        row[...] = jnp.zeros_like(row)
        row[:RANGES, :modes] = value
        col[...] = row[...].T

    def chunk(step, carry):
        base = step * CHUNK
        shift = lax.rem(LANES - base, LANES)
        real = pltpu.roll(col_real[...], shift, 1)
        imag = pltpu.roll(col_imag[...], shift, 1)
        for k in range(CHUNK):
            left_real = jnp.broadcast_to(real[:modes, k : k + 1], (modes, LANES))
            left_imag = jnp.broadcast_to(imag[:modes, k : k + 1], (modes, LANES))
            right_real = row_real[pl.ds(base + k, 1), :]
            right_imag = row_imag[pl.ds(base + k, 1), :]
            even_ref[base + k] = left_real * right_real + left_imag * right_imag
            odd_ref[base + k] = left_real * right_imag - left_imag * right_real
        return carry

    lax.fori_loop(0, RANGES // CHUNK, chunk, 0)


def forms(matrices, weight, tail, sums_ref):
    modes = tail.shape[0]
    depths = tail.shape[1]

    def chunk(step, carry):
        base = step * CHUNK
        left = []
        for k in range(CHUNK):
            high, low = split(matrices(base + k))
            left.append(jnp.concatenate([high, low], 1))
        image = dot(jnp.concatenate(left, 0), weight[...])
        for k in range(CHUNK):
            terms = tail[...] * image[k * modes : (k + 1) * modes]
            sums = jnp.sum(terms.reshape(-1, 8, depths), 0)
            rows = pl.ds(pl.multiple_of((base + k) * 8, 8), 8)
            for half in range(2):
                sums_ref[half, rows, :] = sums[:, half * LANES : (half + 1) * LANES]
        return carry

    lax.fori_loop(0, RANGES // CHUNK, chunk, 0)
    totals = []
    for half in range(2):
        total = sums_ref[half, pl.ds(0, RANGES, stride=8), :]
        for k in range(1, 8):
            total = total + sums_ref[half, pl.ds(k, RANGES, stride=8), :]
        totals.append(total)
    return jnp.concatenate(totals, 1)


def denom_kernel(
    grid_ref, sensor_ref, source_ref, other_ref, even_ref,
    scale_ref, weight_ref, tail_ref, shapes_ref, mixed_ref, whole_ref, sums_ref,
):
    modes = sensor_ref.shape[1]
    mine = grid_ref[0]
    first = mine == 0
    own_shape, other_shape = sensor_ref[mine], other_ref[0]
    own_depth, other_depth = source_ref[mine], other_ref[1]
    whole_ref[...] = jnp.zeros_like(whole_ref)
    whole_ref[:modes, :LANES] = jnp.where(first, own_shape, other_shape)
    whole_ref[:modes, LANES:] = jnp.where(first, other_shape, own_shape)
    shapes = whole_ref[...]
    sensors = shapes.shape[1]
    high, low = split(shapes)
    shapes_ref[:LANES] = high
    shapes_ref[LANES:] = low
    gram = (
        dot(high[:modes], high, ((1,), (1,)))
        + dot(low[:modes], high, ((1,), (1,)))
        + dot(high[:modes], low, ((1,), (1,)))
    )
    source = lax.broadcasted_iota(jnp.int32, (sensors, sensors), 0)
    target = lax.broadcasted_iota(jnp.int32, (sensors, sensors), 1)
    rows = sensors // 4
    order = (source == 4 * (target % rows) + target // rows).astype(jnp.bfloat16)
    mixed_ref[:modes] = dot(high[:modes], order).astype(jnp.bfloat16)
    mixed_ref[modes:] = dot(low[:modes], order).astype(jnp.bfloat16)
    depth = jnp.concatenate(
        [jnp.where(first, own_depth, other_depth), jnp.where(first, other_depth, own_depth)], 1
    )
    depth_high = depth.astype(jnp.bfloat16)
    tail_ref[...] = depth + (depth - depth_high.astype(jnp.float32))
    weight_ref[...] = jnp.zeros_like(weight_ref)
    weight_ref[:modes] = depth_high
    weight_ref[LANES : LANES + modes] = depth_high
    total = forms(lambda j: gram * even_ref[j], weight_ref, tail_ref, sums_ref)
    scale_ref[...] = 1.0 / total


def numer_kernel(
    spectra_ref, scale_ref, weight_ref, tail_ref, shapes_ref, mixed_ref, even_ref, odd_ref,
    power_ref, square_ref, real_ref, imag_ref, sums_ref,
):
    modes = tail_ref.shape[0]
    rows = spectra_ref.shape[0] // 8
    matrix = jnp.concatenate(
        [
            jnp.concatenate([spectra_ref[pl.ds(4 * half + k, rows, stride=8), :] for half in range(2)], 1)
            for k in range(4)
        ],
        0,
    )
    high, low = split(matrix)
    both = dot(mixed_ref[...], high)
    product = both[:modes] + both[modes:] + dot(mixed_ref[:modes], low)
    product_high, product_low = split(product)
    shape_high, shape_low = shapes_ref[:LANES], shapes_ref[LANES:]
    square_ref[...] = jnp.zeros_like(square_ref)
    square_ref[:modes] = (
        dot(product_high, shape_high, ((1,), (1,)))
        + dot(product_low, shape_high, ((1,), (1,)))
        + dot(product_high, shape_low, ((1,), (1,)))
    )
    square = square_ref[...]
    turned = square.T
    real_ref[...] = (0.5 * (square + turned))[:modes]
    imag_ref[...] = (0.5 * (square - turned))[:modes]
    total = forms(
        lambda j: real_ref[...] * even_ref[j] - imag_ref[...] * odd_ref[j], weight_ref, tail_ref, sums_ref
    )
    power = total * scale_ref[...]
    power_ref[pl.ds(0, RANGES, stride=2), :] = power[:, :LANES]
    power_ref[pl.ds(1, RANGES, stride=2), :] = power[:, LANES:]


def shape_of(*shape, dtype=jnp.float32):
    return jax.ShapeDtypeStruct(shape, dtype)


def per_device(cross_spectra, sensor_modes, source_modes, wavenumber, attenuation, mode_counts):
    modes = sensor_modes.shape[1]
    sensors = cross_spectra.shape[3] * 2
    depths = source_modes.shape[2] * 2
    bins = cross_spectra.shape[1]
    mine = lax.axis_index("grid")
    where = mine.reshape(1).astype(jnp.int32)
    other = 1 - mine
    outgoing = jnp.stack(
        [
            lax.dynamic_index_in_dim(sensor_modes, other, 0, False),
            lax.dynamic_index_in_dim(source_modes, other, 0, False),
        ]
    )
    incoming = lax.ppermute(outgoing, "grid", [(0, 1), (1, 0)])
    packed = cross_spectra[0] + cross_spectra[1]
    spectra = lax.all_to_all(packed, ("freq", "grid"), 0, 0, tiled=True)
    even, odd = pl.pallas_call(
        pair_kernel,
        out_shape=[shape_of(RANGES, modes, LANES)] * 2,
        in_specs=[SMEM, SMEM, VMEM, VMEM],
        out_specs=[VMEM] * 2,
        scratch_shapes=[pltpu.VMEM((LANES, LANES), jnp.float32)] * 4,
        cost_estimate=pl.CostEstimate(flops=8_000_000_000, bytes_accessed=0, transcendentals=0),
        name="pairs",
    )(where, mode_counts, wavenumber, attenuation)
    scale, weight, tail, shapes, mixed = pl.pallas_call(
        denom_kernel,
        out_shape=[
            shape_of(RANGES, depths),
            shape_of(2 * LANES, depths, dtype=jnp.bfloat16),
            shape_of(modes, depths),
            shape_of(2 * LANES, sensors, dtype=jnp.bfloat16),
            shape_of(2 * modes, sensors, dtype=jnp.bfloat16),
        ],
        in_specs=[SMEM, VMEM, VMEM, VMEM, VMEM],
        out_specs=[VMEM] * 5,
        scratch_shapes=[pltpu.VMEM((LANES, sensors), jnp.float32), pltpu.VMEM((2, RANGES * 8, LANES), jnp.float32)],
        cost_estimate=pl.CostEstimate(flops=8_000_000_000, bytes_accessed=0, transcendentals=0),
        name="denom",
    )(where, sensor_modes, source_modes, incoming, even)
    power = pl.pallas_call(
        numer_kernel,
        out_shape=shape_of(RANGES * 2, LANES),
        in_specs=[VMEM] * 8,
        out_specs=VMEM,
        scratch_shapes=[
            pltpu.VMEM((LANES, LANES), jnp.float32),
            pltpu.VMEM((modes, LANES), jnp.float32),
            pltpu.VMEM((modes, LANES), jnp.float32),
            pltpu.VMEM((2, RANGES * 8, LANES), jnp.float32),
        ],
        cost_estimate=pl.CostEstimate(flops=8_000_000_000, bytes_accessed=0, transcendentals=0),
        name="numer",
    )(spectra.reshape(-1, LANES), scale, weight, tail, shapes, mixed, even, odd)
    parts = lax.all_to_all(power.reshape(-1, 1, LANES), ("freq", "grid"), 0, 0, tiled=True)
    return jnp.sum(parts.reshape(-1, LANES), 0, keepdims=True) / bins


def solution(mesh):
    placed = (
        P(None, None, "freq", "grid"),
        P("freq", None, "grid"),
        P("freq", None, "grid"),
        P("freq", None),
        P("freq", None),
        P("freq"),
    )
    return jax.shard_map(
        per_device, mesh=mesh, in_specs=placed, out_specs=P("freq", "grid"), check_vma=False
    )
```

```python
import functools

import jax
import jax.numpy as jnp
from jax import lax
from jax.experimental import pallas as pl
from jax.experimental.pallas import tpu as pltpu
from jax.sharding import PartitionSpec as P

RANGES = 64
LANES = 128
CHUNK = 32
CHUNKS = RANGES // CHUNK

VMEM = pl.BlockSpec(memory_space=pltpu.VMEM)
SMEM = pl.BlockSpec(memory_space=pltpu.SMEM)
COST = pl.CostEstimate(flops=8_000_000_000, bytes_accessed=0, transcendentals=0)
PARAMS = pltpu.CompilerParams(vmem_limit_bytes=8 * 1024 * 1024)


def split(value):
    high = value.astype(jnp.bfloat16)
    low = (value - high.astype(jnp.float32)).astype(jnp.bfloat16)
    return high, low


def dot(left, right, contract=((1,), (0,))):
    return lax.dot_general(left, right, (contract, ((), ())), preferred_element_type=jnp.float32)


def pack_kernel(grid_ref, spectra_ref, sensor_ref, source_ref, packed_ref, outgoing_ref):
    packed_ref[...] = spectra_ref[0] + spectra_ref[1]
    outgoing_ref[0] = sensor_ref[0]
    outgoing_ref[1] = source_ref[0]


def forms(matrices, weight, tail, sums_ref):
    modes = tail.shape[0]
    depths = tail.shape[1]

    def chunk(step, carry):
        base = step * CHUNK
        left = []
        for k in range(CHUNK):
            high, low = split(matrices(step, k))
            left.append(jnp.concatenate([high, low], 1))
        image = dot(jnp.concatenate(left, 0), weight[...])
        for k in range(CHUNK):
            terms = tail[...] * image[k * modes : (k + 1) * modes]
            sums = jnp.sum(terms.reshape(-1, 8, depths), 0)
            rows = pl.ds(pl.multiple_of((base + k) * 8, 8), 8)
            for half in range(2):
                sums_ref[half, rows, :] = sums[:, half * LANES : (half + 1) * LANES]
        return carry

    lax.fori_loop(0, CHUNKS, chunk, 0)
    totals = []
    for half in range(2):
        total = sums_ref[half, pl.ds(0, RANGES, stride=8), :]
        for k in range(1, 8):
            total = total + sums_ref[half, pl.ds(k, RANGES, stride=8), :]
        totals.append(total)
    return jnp.concatenate(totals, 1)


def pair(rows_ref, cols_ref, step, k):
    modes = cols_ref.shape[2]
    at = pl.ds(step * CHUNK + k, 1)
    left = [jnp.broadcast_to(cols_ref[part, step, :, k : k + 1], (modes, LANES)) for part in range(2)]
    right = [rows_ref[part, at, :] for part in range(2)]
    return left, right


def denom_kernel(
    bins, grid_ref, counts_ref, wave_ref, atten_ref, sensor_ref, source_ref, other_ref,
    scale_ref, weight_ref, tail_ref, shapes_ref, mixed_ref, rows_ref, cols_ref, whole_ref, sums_ref,
):
    modes = sensor_ref.shape[1]
    mine = grid_ref[0]
    first = mine == 0
    count = counts_ref[mine]

    ranges = 1.0 + lax.broadcasted_iota(jnp.int32, (RANGES, modes), 0).astype(jnp.float32)
    phase = wave_ref[pl.ds(mine, 1), :] * ranges
    magnitude = jnp.exp(-atten_ref[pl.ds(mine, 1), :] * ranges) / jnp.sqrt(phase)
    keep = lax.broadcasted_iota(jnp.int32, (RANGES, modes), 1) < count
    magnitude = jnp.where(keep, magnitude, 0.0)
    rows_ref[...] = jnp.zeros_like(rows_ref)
    for part, value in enumerate((magnitude * jnp.cos(phase), magnitude * jnp.sin(phase))):
        rows_ref[part, :RANGES, :modes] = value
        turned = rows_ref[part].T
        for step in range(CHUNKS):
            moved = pltpu.roll(turned, LANES - CHUNK * step, 1) if step else turned
            cols_ref[part, step] = moved[:modes]

    own_shape, other_shape = sensor_ref[mine], other_ref[0]
    own_depth, other_depth = source_ref[mine], other_ref[1]
    whole_ref[...] = jnp.zeros_like(whole_ref)
    whole_ref[:modes, :LANES] = jnp.where(first, own_shape, other_shape)
    whole_ref[:modes, LANES:] = jnp.where(first, other_shape, own_shape)
    shapes = whole_ref[...]
    sensors = shapes.shape[1]
    high, low = split(shapes)
    shapes_ref[:LANES] = high
    shapes_ref[LANES:] = low
    gram = (
        dot(high[:modes], high, ((1,), (1,)))
        + dot(low[:modes], high, ((1,), (1,)))
        + dot(high[:modes], low, ((1,), (1,)))
    )
    source = lax.broadcasted_iota(jnp.int32, (sensors, sensors), 0)
    target = lax.broadcasted_iota(jnp.int32, (sensors, sensors), 1)
    rows = sensors // 4
    order = (source == 4 * (target % rows) + target // rows).astype(jnp.bfloat16)
    mixed_ref[:modes] = dot(high[:modes], order).astype(jnp.bfloat16)
    mixed_ref[modes:] = dot(low[:modes], order).astype(jnp.bfloat16)
    depth = jnp.concatenate(
        [jnp.where(first, own_depth, other_depth), jnp.where(first, other_depth, own_depth)], 1
    )
    depth_high = depth.astype(jnp.bfloat16)
    tail_ref[...] = depth + (depth - depth_high.astype(jnp.float32))
    weight_ref[...] = jnp.zeros_like(weight_ref)
    weight_ref[:modes] = depth_high
    weight_ref[LANES : LANES + modes] = depth_high

    def matrices(step, k):
        (left_real, left_imag), (right_real, right_imag) = pair(rows_ref, cols_ref, step, k)
        return gram * (left_real * right_real + left_imag * right_imag)

    total = forms(matrices, weight_ref, tail_ref, sums_ref)
    scale_ref[...] = 1.0 / (total * bins)


def numer_kernel(
    spectra_ref, scale_ref, weight_ref, tail_ref, shapes_ref, mixed_ref, rows_ref, cols_ref,
    power_ref, square_ref, real_ref, imag_ref, sums_ref,
):
    modes = tail_ref.shape[0]
    rows = spectra_ref.shape[0] // 8
    matrix = jnp.concatenate(
        [
            jnp.concatenate([spectra_ref[pl.ds(4 * half + k, rows, stride=8), :] for half in range(2)], 1)
            for k in range(4)
        ],
        0,
    )
    high, low = split(matrix)
    both = dot(mixed_ref[...], high)
    product = both[:modes] + both[modes:] + dot(mixed_ref[:modes], low)
    product_high, product_low = split(product)
    shape_high, shape_low = shapes_ref[:LANES], shapes_ref[LANES:]
    square_ref[...] = jnp.zeros_like(square_ref)
    square_ref[:modes] = (
        dot(product_high, shape_high, ((1,), (1,)))
        + dot(product_low, shape_high, ((1,), (1,)))
        + dot(product_high, shape_low, ((1,), (1,)))
    )
    square = square_ref[...]
    turned = square.T
    real_ref[...] = (0.5 * (square + turned))[:modes]
    imag_ref[...] = (0.5 * (square - turned))[:modes]

    def matrices(step, k):
        (left_real, left_imag), (right_real, right_imag) = pair(rows_ref, cols_ref, step, k)
        even = left_real * right_real + left_imag * right_imag
        odd = left_real * right_imag - left_imag * right_real
        return real_ref[...] * even - imag_ref[...] * odd

    power = forms(matrices, weight_ref, tail_ref, sums_ref) * scale_ref[...]
    power_ref[pl.ds(0, RANGES, stride=2), :] = power[:, :LANES]
    power_ref[pl.ds(1, RANGES, stride=2), :] = power[:, LANES:]


def shape_of(*shape, dtype=jnp.float32):
    return jax.ShapeDtypeStruct(shape, dtype)


def per_device(cross_spectra, sensor_modes, source_modes, wavenumber, attenuation, mode_counts):
    modes = sensor_modes.shape[1]
    sensors = cross_spectra.shape[3] * 2
    depths = source_modes.shape[2] * 2
    bins = cross_spectra.shape[1]
    mine = lax.axis_index("grid").astype(jnp.int32)
    where = mine.reshape(1)
    steps = 4
    block = bins * 4 // steps
    packed, outgoing = pl.pallas_call(
        pack_kernel,
        grid_spec=pltpu.PrefetchScalarGridSpec(
            num_scalar_prefetch=1,
            grid=(steps,),
            in_specs=[
                pl.BlockSpec((2, block, LANES), lambda i, at: (0, i, 0)),
                pl.BlockSpec((1, modes, LANES), lambda i, at: (1 - at[0], 0, 0)),
                pl.BlockSpec((1, modes, LANES), lambda i, at: (1 - at[0], 0, 0)),
            ],
            out_specs=[
                pl.BlockSpec((block, LANES), lambda i, at: (i, 0)),
                pl.BlockSpec((2, modes, LANES), lambda i, at: (0, 0, 0)),
            ],
        ),
        out_shape=[shape_of(bins * 4, LANES), shape_of(2, modes, LANES)],
        name="pack",
    )(where, cross_spectra.reshape(2, bins * 4, LANES), sensor_modes, source_modes)
    incoming = lax.ppermute(outgoing, "grid", [(0, 1), (1, 0)])
    spectra = lax.all_to_all(packed.reshape(bins, 4, LANES), ("freq", "grid"), 0, 0, tiled=True)
    tables = pl.pallas_call(
        functools.partial(denom_kernel, bins),
        out_shape=[
            shape_of(RANGES, depths),
            shape_of(2 * LANES, depths, dtype=jnp.bfloat16),
            shape_of(modes, depths),
            shape_of(2 * LANES, sensors, dtype=jnp.bfloat16),
            shape_of(2 * modes, sensors, dtype=jnp.bfloat16),
            shape_of(2, LANES, LANES),
            shape_of(2, CHUNKS, modes, LANES),
        ],
        in_specs=[SMEM, SMEM, VMEM, VMEM, VMEM, VMEM, VMEM],
        out_specs=[VMEM] * 7,
        scratch_shapes=[
            pltpu.VMEM((LANES, sensors), jnp.float32),
            pltpu.VMEM((2, RANGES * 8, LANES), jnp.float32),
        ],
        cost_estimate=COST,
        compiler_params=PARAMS,
        name="denom",
    )(where, mode_counts, wavenumber, attenuation, sensor_modes, source_modes, incoming)
    power = pl.pallas_call(
        numer_kernel,
        out_shape=shape_of(RANGES * 2, LANES),
        in_specs=[VMEM] * 8,
        out_specs=VMEM,
        scratch_shapes=[
            pltpu.VMEM((LANES, LANES), jnp.float32),
            pltpu.VMEM((modes, LANES), jnp.float32),
            pltpu.VMEM((modes, LANES), jnp.float32),
            pltpu.VMEM((2, RANGES * 8, LANES), jnp.float32),
        ],
        cost_estimate=COST,
        compiler_params=PARAMS,
        name="numer",
    )(spectra.reshape(-1, LANES), *tables)
    parts = lax.all_to_all(power.reshape(-1, 1, LANES), ("freq", "grid"), 0, 0, tiled=True)
    return jnp.sum(parts.reshape(-1, LANES), 0, keepdims=True)


def solution(mesh):
    placed = (
        P(None, None, "freq", "grid"),
        P("freq", None, "grid"),
        P("freq", None, "grid"),
        P("freq", None),
        P("freq", None),
        P("freq"),
    )
    return jax.shard_map(
        per_device, mesh=mesh, in_specs=placed, out_specs=P("freq", "grid"), check_vma=False
    )
```

```python
import functools

import jax
import jax.numpy as jnp
from jax import lax
from jax.experimental import pallas as pl
from jax.experimental.pallas import tpu as pltpu
from jax.sharding import PartitionSpec as P

RANGES = 64
LANES = 128
CHUNK = 32
PIECES = 2
CHUNKS = RANGES // CHUNK

VMEM = pl.BlockSpec(memory_space=pltpu.VMEM)
ANY = pl.BlockSpec(memory_space=pl.ANY)
SMEM = pl.BlockSpec(memory_space=pltpu.SMEM)
COST = pl.CostEstimate(flops=8_000_000_000, bytes_accessed=0, transcendentals=0)
PARAMS = pltpu.CompilerParams(vmem_limit_bytes=8 * 1024 * 1024)


def split(value):
    high = value.astype(jnp.bfloat16)
    low = (value - high.astype(jnp.float32)).astype(jnp.bfloat16)
    return high, low


def dot(left, right, contract=((1,), (0,))):
    return lax.dot_general(left, right, (contract, ((), ())), preferred_element_type=jnp.float32)


def pack_kernel(
    grid_ref, spectra_ref, sensor_ref, source_ref, packed_ref, outgoing_ref, both_ref, sum_ref, half_ref, in_sem, out_sem
):
    other = 1 - grid_ref[0]
    rows = packed_ref.shape[0] // PIECES
    halves = [
        pltpu.make_async_copy(ref.at[other], half_ref.at[k], in_sem.at[PIECES + k])
        for k, ref in enumerate((sensor_ref, source_ref))
    ]
    pieces = [
        pltpu.make_async_copy(spectra_ref.at[:, pl.ds(k * rows, rows)], both_ref.at[k], in_sem.at[k])
        for k in range(PIECES)
    ]
    for copy in halves + pieces:
        copy.start()
    sends = []
    for k, copy in enumerate(halves):
        copy.wait()
        sends.append(pltpu.make_async_copy(half_ref.at[k], outgoing_ref.at[k], out_sem.at[PIECES + k]))
        sends[-1].start()
    for k, copy in enumerate(pieces):
        copy.wait()
        sum_ref[k] = both_ref[k, 0] + both_ref[k, 1]
        sends.append(pltpu.make_async_copy(sum_ref.at[k], packed_ref.at[pl.ds(k * rows, rows)], out_sem.at[k]))
        sends[-1].start()
    for copy in sends:
        copy.wait()


def forms(matrices, weight, tail, sums_ref):
    modes = tail.shape[0]
    depths = tail.shape[1]

    def chunk(step, carry):
        base = step * CHUNK
        left = []
        for k in range(CHUNK):
            high, low = split(matrices(step, k))
            left.append(jnp.concatenate([high, low], 1))
        image = dot(jnp.concatenate(left, 0), weight[...])
        for k in range(CHUNK):
            terms = tail[...] * image[k * modes : (k + 1) * modes]
            sums = jnp.sum(terms.reshape(-1, 8, depths), 0)
            rows = pl.ds(pl.multiple_of((base + k) * 8, 8), 8)
            for half in range(2):
                sums_ref[half, rows, :] = sums[:, half * LANES : (half + 1) * LANES]
        return carry

    lax.fori_loop(0, CHUNKS, chunk, 0)
    totals = []
    for half in range(2):
        total = sums_ref[half, pl.ds(0, RANGES, stride=8), :]
        for k in range(1, 8):
            total = total + sums_ref[half, pl.ds(k, RANGES, stride=8), :]
        totals.append(total)
    return jnp.concatenate(totals, 1)


def pair(rows_ref, cols_ref, step, k):
    modes = cols_ref.shape[2]
    at = pl.ds(step * CHUNK + k, 1)
    left = [jnp.broadcast_to(cols_ref[part, step, :, k : k + 1], (modes, LANES)) for part in range(2)]
    right = [rows_ref[part, at, :] for part in range(2)]
    return left, right


def denom_kernel(
    bins, grid_ref, counts_ref, wave_ref, atten_ref, sensor_ref, source_ref, other_ref,
    scale_ref, weight_ref, tail_ref, shapes_ref, mixed_ref, rows_ref, cols_ref, whole_ref, sums_ref,
):
    modes = sensor_ref.shape[1]
    mine = grid_ref[0]
    first = mine == 0
    count = counts_ref[mine]

    ranges = 1.0 + lax.broadcasted_iota(jnp.int32, (RANGES, modes), 0).astype(jnp.float32)
    phase = wave_ref[pl.ds(mine, 1), :] * ranges
    magnitude = jnp.exp(-atten_ref[pl.ds(mine, 1), :] * ranges) / jnp.sqrt(phase)
    keep = lax.broadcasted_iota(jnp.int32, (RANGES, modes), 1) < count
    magnitude = jnp.where(keep, magnitude, 0.0)
    rows_ref[...] = jnp.zeros_like(rows_ref)
    for part, value in enumerate((magnitude * jnp.cos(phase), magnitude * jnp.sin(phase))):
        rows_ref[part, :RANGES, :modes] = value
        turned = rows_ref[part].T
        for step in range(CHUNKS):
            moved = pltpu.roll(turned, LANES - CHUNK * step, 1) if step else turned
            cols_ref[part, step] = moved[:modes]

    own_shape, other_shape = sensor_ref[mine], other_ref[0]
    own_depth, other_depth = source_ref[mine], other_ref[1]
    whole_ref[...] = jnp.zeros_like(whole_ref)
    whole_ref[:modes, :LANES] = jnp.where(first, own_shape, other_shape)
    whole_ref[:modes, LANES:] = jnp.where(first, other_shape, own_shape)
    shapes = whole_ref[...]
    sensors = shapes.shape[1]
    high, low = split(shapes)
    shapes_ref[:LANES] = high
    shapes_ref[LANES:] = low
    gram = (
        dot(high[:modes], high, ((1,), (1,)))
        + dot(low[:modes], high, ((1,), (1,)))
        + dot(high[:modes], low, ((1,), (1,)))
    )
    source = lax.broadcasted_iota(jnp.int32, (sensors, sensors), 0)
    target = lax.broadcasted_iota(jnp.int32, (sensors, sensors), 1)
    rows = sensors // 4
    order = (source == 4 * (target % rows) + target // rows).astype(jnp.bfloat16)
    mixed_ref[:modes] = dot(high[:modes], order).astype(jnp.bfloat16)
    mixed_ref[modes:] = dot(low[:modes], order).astype(jnp.bfloat16)
    depth = jnp.concatenate(
        [jnp.where(first, own_depth, other_depth), jnp.where(first, other_depth, own_depth)], 1
    )
    depth_high = depth.astype(jnp.bfloat16)
    tail_ref[...] = depth + (depth - depth_high.astype(jnp.float32))
    weight_ref[...] = jnp.zeros_like(weight_ref)
    weight_ref[:modes] = depth_high
    weight_ref[LANES : LANES + modes] = depth_high

    def matrices(step, k):
        (left_real, left_imag), (right_real, right_imag) = pair(rows_ref, cols_ref, step, k)
        return gram * (left_real * right_real + left_imag * right_imag)

    total = forms(matrices, weight_ref, tail_ref, sums_ref)
    scale_ref[...] = 1.0 / (total * bins)


def numer_kernel(
    spectra_ref, scale_ref, weight_ref, tail_ref, shapes_ref, mixed_ref, rows_ref, cols_ref,
    power_ref, square_ref, real_ref, imag_ref, sums_ref,
):
    modes = tail_ref.shape[0]
    rows = spectra_ref.shape[0] // 8
    matrix = jnp.concatenate(
        [
            jnp.concatenate([spectra_ref[pl.ds(4 * half + k, rows, stride=8), :] for half in range(2)], 1)
            for k in range(4)
        ],
        0,
    )
    high, low = split(matrix)
    both = dot(mixed_ref[...], high)
    product = both[:modes] + both[modes:] + dot(mixed_ref[:modes], low)
    product_high, product_low = split(product)
    shape_high, shape_low = shapes_ref[:LANES], shapes_ref[LANES:]
    square_ref[...] = jnp.zeros_like(square_ref)
    square_ref[:modes] = (
        dot(product_high, shape_high, ((1,), (1,)))
        + dot(product_low, shape_high, ((1,), (1,)))
        + dot(product_high, shape_low, ((1,), (1,)))
    )
    square = square_ref[...]
    turned = square.T
    real_ref[...] = (0.5 * (square + turned))[:modes]
    imag_ref[...] = (0.5 * (square - turned))[:modes]

    def matrices(step, k):
        (left_real, left_imag), (right_real, right_imag) = pair(rows_ref, cols_ref, step, k)
        even = left_real * right_real + left_imag * right_imag
        odd = left_real * right_imag - left_imag * right_real
        return real_ref[...] * even - imag_ref[...] * odd

    power = forms(matrices, weight_ref, tail_ref, sums_ref) * scale_ref[...]
    power_ref[pl.ds(0, RANGES, stride=2), :] = power[:, :LANES]
    power_ref[pl.ds(1, RANGES, stride=2), :] = power[:, LANES:]


def shape_of(*shape, dtype=jnp.float32):
    return jax.ShapeDtypeStruct(shape, dtype)


def per_device(cross_spectra, sensor_modes, source_modes, wavenumber, attenuation, mode_counts):
    modes = sensor_modes.shape[1]
    sensors = cross_spectra.shape[3] * 2
    depths = source_modes.shape[2] * 2
    bins = cross_spectra.shape[1]
    mine = lax.axis_index("grid").astype(jnp.int32)
    where = mine.reshape(1)
    rows = bins * 4 // PIECES
    packed, outgoing = pl.pallas_call(
        pack_kernel,
        out_shape=[shape_of(bins * 4, LANES), shape_of(2, modes, LANES)],
        in_specs=[SMEM, ANY, ANY, ANY],
        out_specs=[ANY] * 2,
        scratch_shapes=[
            pltpu.VMEM((PIECES, 2, rows, LANES), jnp.float32),
            pltpu.VMEM((PIECES, rows, LANES), jnp.float32),
            pltpu.VMEM((2, modes, LANES), jnp.float32),
            pltpu.SemaphoreType.DMA((PIECES + 2,)),
            pltpu.SemaphoreType.DMA((PIECES + 2,)),
        ],
        name="pack",
    )(where, cross_spectra.reshape(2, bins * 4, LANES), sensor_modes, source_modes)
    incoming = lax.ppermute(outgoing, "grid", [(0, 1), (1, 0)])
    spectra = lax.all_to_all(packed.reshape(bins, 4, LANES), ("freq", "grid"), 0, 0, tiled=True)
    tables = pl.pallas_call(
        functools.partial(denom_kernel, bins),
        out_shape=[
            shape_of(RANGES, depths),
            shape_of(2 * LANES, depths, dtype=jnp.bfloat16),
            shape_of(modes, depths),
            shape_of(2 * LANES, sensors, dtype=jnp.bfloat16),
            shape_of(2 * modes, sensors, dtype=jnp.bfloat16),
            shape_of(2, LANES, LANES),
            shape_of(2, CHUNKS, modes, LANES),
        ],
        in_specs=[SMEM, SMEM, VMEM, VMEM, VMEM, VMEM, VMEM],
        out_specs=[VMEM] * 7,
        scratch_shapes=[pltpu.VMEM((LANES, sensors), jnp.float32), pltpu.VMEM((2, RANGES * 8, LANES), jnp.float32)],
        cost_estimate=COST,
        compiler_params=PARAMS,
        name="denom",
    )(where, mode_counts, wavenumber, attenuation, sensor_modes, source_modes, incoming)
    power = pl.pallas_call(
        numer_kernel,
        out_shape=shape_of(RANGES * 2, LANES),
        in_specs=[VMEM] * 8,
        out_specs=VMEM,
        scratch_shapes=[
            pltpu.VMEM((LANES, LANES), jnp.float32),
            pltpu.VMEM((modes, LANES), jnp.float32),
            pltpu.VMEM((modes, LANES), jnp.float32),
            pltpu.VMEM((2, RANGES * 8, LANES), jnp.float32),
        ],
        cost_estimate=COST,
        compiler_params=PARAMS,
        name="numer",
    )(spectra.reshape(-1, LANES), *tables)
    parts = lax.all_to_all(power.reshape(-1, 1, LANES), ("freq", "grid"), 0, 0, tiled=True)
    return jnp.sum(parts.reshape(-1, LANES), 0, keepdims=True)


def solution(mesh):
    placed = (
        P(None, None, "freq", "grid"),
        P("freq", None, "grid"),
        P("freq", None, "grid"),
        P("freq", None),
        P("freq", None),
        P("freq"),
    )
    return jax.shard_map(
        per_device, mesh=mesh, in_specs=placed, out_specs=P("freq", "grid"), check_vma=False
    )
```

```python
import functools

import jax
import jax.numpy as jnp
from jax import lax
from jax.experimental import pallas as pl
from jax.experimental.pallas import tpu as pltpu
from jax.sharding import PartitionSpec as P

RANGES = 64
LANES = 128
CHUNK = 16
PIECES = 2

VMEM = pl.BlockSpec(memory_space=pltpu.VMEM)
ANY = pl.BlockSpec(memory_space=pl.ANY)
SMEM = pl.BlockSpec(memory_space=pltpu.SMEM)
COST = pl.CostEstimate(flops=8_000_000_000, bytes_accessed=0, transcendentals=0)
PARAMS = pltpu.CompilerParams(vmem_limit_bytes=8 * 1024 * 1024)


def split(value):
    high = value.astype(jnp.bfloat16)
    low = (value - high.astype(jnp.float32)).astype(jnp.bfloat16)
    return high, low


def dot(left, right, contract=((1,), (0,))):
    return lax.dot_general(left, right, (contract, ((), ())), preferred_element_type=jnp.float32)


def pack_kernel(
    grid_ref, spectra_ref, sensor_ref, source_ref, packed_ref, outgoing_ref, both_ref, sum_ref, half_ref, in_sem, out_sem
):
    other = 1 - grid_ref[0]
    rows = packed_ref.shape[0] // PIECES
    halves = [
        pltpu.make_async_copy(ref.at[other], half_ref.at[k], in_sem.at[PIECES + k])
        for k, ref in enumerate((sensor_ref, source_ref))
    ]
    pieces = [
        pltpu.make_async_copy(spectra_ref.at[:, pl.ds(k * rows, rows)], both_ref.at[k], in_sem.at[k])
        for k in range(PIECES)
    ]
    for copy in halves + pieces:
        copy.start()
    sends = []
    for k, copy in enumerate(halves):
        copy.wait()
        sends.append(pltpu.make_async_copy(half_ref.at[k], outgoing_ref.at[k], out_sem.at[PIECES + k]))
        sends[-1].start()
    for k, copy in enumerate(pieces):
        copy.wait()
        sum_ref[k] = both_ref[k, 0] + both_ref[k, 1]
        sends.append(pltpu.make_async_copy(sum_ref.at[k], packed_ref.at[pl.ds(k * rows, rows)], out_sem.at[k]))
        sends[-1].start()
    for copy in sends:
        copy.wait()


def forms(exact, twice_ref, square_ref, weight, tail, sums_ref):
    modes = tail.shape[0]
    depths = tail.shape[1]
    for base in range(0, RANGES, CHUNK):
        left = []
        before = now = None
        for j in range(base, base + CHUNK):
            if j < base + 2:
                later = exact(j)
            else:
                later = twice_ref[...] * now - square_ref[...] * before
            before, now = now, later
            high, low = split(now)
            left.append(jnp.concatenate([high, low], 1))
        image = dot(jnp.concatenate(left, 0), weight[...])
        for k in range(CHUNK):
            terms = tail[...] * image[k * modes : (k + 1) * modes]
            sums = jnp.sum(terms.reshape(-1, 8, depths), 0)
            row = (base + k) * 8
            for half in range(2):
                sums_ref[half, row : row + 8, :] = sums[:, half * LANES : (half + 1) * LANES]
    totals = []
    for half in range(2):
        total = sums_ref[half, pl.ds(0, RANGES, stride=8), :]
        for k in range(1, 8):
            total = total + sums_ref[half, pl.ds(k, RANGES, stride=8), :]
        totals.append(total)
    return jnp.concatenate(totals, 1)


def pair(rows_ref, cols_ref, j):
    modes = cols_ref.shape[1]
    left = [jnp.broadcast_to(cols_ref[part, :, j : j + 1], (modes, LANES)) for part in range(2)]
    right = [rows_ref[part, j : j + 1, :] for part in range(2)]
    return left, right


def denom_kernel(
    bins, grid_ref, counts_ref, wave_ref, atten_ref, sensor_ref, source_ref, other_ref,
    scale_ref, weight_ref, tail_ref, shapes_ref, mixed_ref, rows_ref, cols_ref, twice_ref, square_ref,
    whole_ref, spread_ref, sums_ref,
):
    modes = sensor_ref.shape[1]
    mine = grid_ref[0]
    first = mine == 0
    count = counts_ref[mine]

    wave = wave_ref[pl.ds(mine, 1), :]
    atten = atten_ref[pl.ds(mine, 1), :]
    ranges = 1.0 + lax.broadcasted_iota(jnp.int32, (RANGES, modes), 0).astype(jnp.float32)
    phase = wave * ranges
    keep = lax.broadcasted_iota(jnp.int32, (RANGES, modes), 1) < count
    magnitude = jnp.where(keep, jnp.exp(-atten * ranges) / jnp.sqrt(wave), 0.0)
    rows_ref[...] = jnp.zeros_like(rows_ref)
    for part, value in enumerate((magnitude * jnp.cos(phase), magnitude * jnp.sin(phase))):
        rows_ref[part, :RANGES, :modes] = value
        cols_ref[part] = rows_ref[part].T[:modes]
    spread_ref[...] = jnp.zeros_like(spread_ref)
    spread_ref[0, :, :modes] = jnp.broadcast_to(wave, (LANES, modes))
    spread_ref[1, :, :modes] = jnp.broadcast_to(atten, (LANES, modes))
    waves, attens = spread_ref[0], spread_ref[1]
    decay = jnp.exp(-(attens.T + attens))
    twice_ref[...] = (2.0 * decay * jnp.cos(waves - waves.T))[:modes]
    square_ref[...] = (decay * decay)[:modes]

    own_shape, other_shape = sensor_ref[mine], other_ref[0]
    own_depth, other_depth = source_ref[mine], other_ref[1]
    whole_ref[...] = jnp.zeros_like(whole_ref)
    whole_ref[:modes, :LANES] = jnp.where(first, own_shape, other_shape)
    whole_ref[:modes, LANES:] = jnp.where(first, other_shape, own_shape)
    shapes = whole_ref[...]
    sensors = shapes.shape[1]
    high, low = split(shapes)
    shapes_ref[:LANES] = high
    shapes_ref[LANES:] = low
    gram = (
        dot(high[:modes], high, ((1,), (1,)))
        + dot(low[:modes], high, ((1,), (1,)))
        + dot(high[:modes], low, ((1,), (1,)))
    )
    source = lax.broadcasted_iota(jnp.int32, (sensors, sensors), 0)
    target = lax.broadcasted_iota(jnp.int32, (sensors, sensors), 1)
    rows = sensors // 4
    order = (source == 4 * (target % rows) + target // rows).astype(jnp.bfloat16)
    mixed_ref[:modes] = dot(high[:modes], order).astype(jnp.bfloat16)
    mixed_ref[modes:] = dot(low[:modes], order).astype(jnp.bfloat16)
    depth = jnp.concatenate(
        [jnp.where(first, own_depth, other_depth), jnp.where(first, other_depth, own_depth)], 1
    )
    depth_high = depth.astype(jnp.bfloat16)
    tail_ref[...] = depth + (depth - depth_high.astype(jnp.float32))
    weight_ref[...] = jnp.zeros_like(weight_ref)
    weight_ref[:modes] = depth_high
    weight_ref[LANES : LANES + modes] = depth_high

    def exact(j):
        (left_real, left_imag), (right_real, right_imag) = pair(rows_ref, cols_ref, j)
        return gram * (left_real * right_real + left_imag * right_imag)

    total = forms(exact, twice_ref, square_ref, weight_ref, tail_ref, sums_ref)
    scale_ref[...] = 1.0 / (total * bins)


def numer_kernel(
    spectra_ref, scale_ref, weight_ref, tail_ref, shapes_ref, mixed_ref, rows_ref, cols_ref, twice_ref, square_ref,
    power_ref, whole_ref, real_ref, imag_ref, sums_ref,
):
    modes = tail_ref.shape[0]
    rows = spectra_ref.shape[0] // 8
    matrix = jnp.concatenate(
        [
            jnp.concatenate([spectra_ref[pl.ds(4 * half + k, rows, stride=8), :] for half in range(2)], 1)
            for k in range(4)
        ],
        0,
    )
    high, low = split(matrix)
    both = dot(mixed_ref[...], high)
    product = both[:modes] + both[modes:] + dot(mixed_ref[:modes], low)
    product_high, product_low = split(product)
    shape_high, shape_low = shapes_ref[:LANES], shapes_ref[LANES:]
    whole_ref[...] = jnp.zeros_like(whole_ref)
    whole_ref[:modes] = (
        dot(product_high, shape_high, ((1,), (1,)))
        + dot(product_low, shape_high, ((1,), (1,)))
        + dot(product_high, shape_low, ((1,), (1,)))
    )
    square = whole_ref[...]
    turned = square.T
    real_ref[...] = (0.5 * (square + turned))[:modes]
    imag_ref[...] = (0.5 * (square - turned))[:modes]

    def exact(j):
        (left_real, left_imag), (right_real, right_imag) = pair(rows_ref, cols_ref, j)
        even = left_real * right_real + left_imag * right_imag
        odd = left_real * right_imag - left_imag * right_real
        return real_ref[...] * even - imag_ref[...] * odd

    power = forms(exact, twice_ref, square_ref, weight_ref, tail_ref, sums_ref) * scale_ref[...]
    power_ref[pl.ds(0, RANGES, stride=2), :] = power[:, :LANES]
    power_ref[pl.ds(1, RANGES, stride=2), :] = power[:, LANES:]


def shape_of(*shape, dtype=jnp.float32):
    return jax.ShapeDtypeStruct(shape, dtype)


def per_device(cross_spectra, sensor_modes, source_modes, wavenumber, attenuation, mode_counts):
    modes = sensor_modes.shape[1]
    sensors = cross_spectra.shape[3] * 2
    depths = source_modes.shape[2] * 2
    bins = cross_spectra.shape[1]
    mine = lax.axis_index("grid").astype(jnp.int32)
    where = mine.reshape(1)
    rows = bins * 4 // PIECES
    packed, outgoing = pl.pallas_call(
        pack_kernel,
        out_shape=[shape_of(bins * 4, LANES), shape_of(2, modes, LANES)],
        in_specs=[SMEM, ANY, ANY, ANY],
        out_specs=[ANY] * 2,
        scratch_shapes=[
            pltpu.VMEM((PIECES, 2, rows, LANES), jnp.float32),
            pltpu.VMEM((PIECES, rows, LANES), jnp.float32),
            pltpu.VMEM((2, modes, LANES), jnp.float32),
            pltpu.SemaphoreType.DMA((PIECES + 2,)),
            pltpu.SemaphoreType.DMA((PIECES + 2,)),
        ],
        name="pack",
    )(where, cross_spectra.reshape(2, bins * 4, LANES), sensor_modes, source_modes)
    incoming = lax.ppermute(outgoing, "grid", [(0, 1), (1, 0)])
    spectra = lax.all_to_all(packed.reshape(bins, 4, LANES), ("freq", "grid"), 0, 0, tiled=True)
    tables = pl.pallas_call(
        functools.partial(denom_kernel, bins),
        out_shape=[
            shape_of(RANGES, depths),
            shape_of(2 * LANES, depths, dtype=jnp.bfloat16),
            shape_of(modes, depths),
            shape_of(2 * LANES, sensors, dtype=jnp.bfloat16),
            shape_of(2 * modes, sensors, dtype=jnp.bfloat16),
            shape_of(2, LANES, LANES),
            shape_of(2, modes, LANES),
            shape_of(modes, LANES),
            shape_of(modes, LANES),
        ],
        in_specs=[SMEM, SMEM, VMEM, VMEM, VMEM, VMEM, VMEM],
        out_specs=[VMEM] * 9,
        scratch_shapes=[
            pltpu.VMEM((LANES, sensors), jnp.float32),
            pltpu.VMEM((2, LANES, LANES), jnp.float32),
            pltpu.VMEM((2, RANGES * 8, LANES), jnp.float32),
        ],
        cost_estimate=COST,
        compiler_params=PARAMS,
        name="denom",
    )(where, mode_counts, wavenumber, attenuation, sensor_modes, source_modes, incoming)
    power = pl.pallas_call(
        numer_kernel,
        out_shape=shape_of(RANGES * 2, LANES),
        in_specs=[VMEM] * 10,
        out_specs=VMEM,
        scratch_shapes=[
            pltpu.VMEM((LANES, LANES), jnp.float32),
            pltpu.VMEM((modes, LANES), jnp.float32),
            pltpu.VMEM((modes, LANES), jnp.float32),
            pltpu.VMEM((2, RANGES * 8, LANES), jnp.float32),
        ],
        cost_estimate=COST,
        compiler_params=PARAMS,
        name="numer",
    )(spectra.reshape(-1, LANES), *tables)
    parts = lax.all_to_all(power.reshape(-1, 1, LANES), ("freq", "grid"), 0, 0, tiled=True)
    return jnp.sum(parts.reshape(-1, LANES), 0, keepdims=True)


def solution(mesh):
    placed = (
        P(None, None, "freq", "grid"),
        P("freq", None, "grid"),
        P("freq", None, "grid"),
        P("freq", None),
        P("freq", None),
        P("freq"),
    )
    return jax.shard_map(
        per_device, mesh=mesh, in_specs=placed, out_specs=P("freq", "grid"), check_vma=False
    )
```

```python
import functools

import jax
import jax.numpy as jnp
from jax import lax
from jax.experimental import pallas as pl
from jax.experimental.pallas import tpu as pltpu
from jax.sharding import PartitionSpec as P


RANGES = 64
LANES = 128
CHUNK = 32

VMEM = pl.BlockSpec(memory_space=pltpu.VMEM)
HBM = pl.BlockSpec(memory_space=pltpu.HBM)
SMEM = pl.BlockSpec(memory_space=pltpu.SMEM)
COST = pl.CostEstimate(flops=8_000_000_000, bytes_accessed=0, transcendentals=0)
PARAMS = pltpu.CompilerParams(vmem_limit_bytes=8 * 1024 * 1024)


def split(value):
    high = value.astype(jnp.bfloat16)
    low = (value - high.astype(jnp.float32)).astype(jnp.bfloat16)
    return high, low


def dot(left, right, contract=((1,), (0,))):
    return lax.dot_general(left, right, (contract, ((), ())), preferred_element_type=jnp.float32)


def halves_kernel(sensor_ref, source_ref, outgoing_ref, sem):
    other = 1 - lax.axis_index("grid")
    copies = [
        pltpu.make_async_copy(ref.at[other], outgoing_ref.at[k], sem.at[k])
        for k, ref in enumerate((sensor_ref, source_ref))
    ]
    for copy in copies:
        copy.start()
    for copy in copies:
        copy.wait()


def pack_kernel(spectra_ref, packed_ref):
    packed_ref[...] = spectra_ref[0] + spectra_ref[1]


def forms(exact, twice_ref, square_ref, weight, tail, sums_ref):
    modes = tail.shape[0]
    depths = tail.shape[1]
    for base in range(0, RANGES, CHUNK):
        left = []
        before = now = None
        for j in range(base, base + CHUNK):
            if j < base + 2:
                later = exact(j)
            else:
                later = twice_ref[...] * now - square_ref[...] * before
            before, now = now, later
            high, low = split(now)
            left.append(jnp.concatenate([high, low], 1))
        image = dot(jnp.concatenate(left, 0), weight[...])
        for k in range(CHUNK):
            terms = tail[...] * image[k * modes : (k + 1) * modes]
            sums = jnp.sum(terms.reshape(-1, 8, depths), 0)
            row = (base + k) * 8
            for half in range(2):
                sums_ref[half, row : row + 8, :] = sums[:, half * LANES : (half + 1) * LANES]
    totals = []
    for half in range(2):
        total = sums_ref[half, pl.ds(0, RANGES, stride=8), :]
        for k in range(1, 8):
            total = total + sums_ref[half, pl.ds(k, RANGES, stride=8), :]
        totals.append(total)
    return jnp.concatenate(totals, 1)


def pair(rows_ref, cols_ref, j):
    modes = cols_ref.shape[1]
    left = [jnp.broadcast_to(cols_ref[part, :, j : j + 1], (modes, LANES)) for part in range(2)]
    right = [rows_ref[part, j : j + 1, :] for part in range(2)]
    return left, right


def denom_kernel(
    bins, grid_ref, counts_ref, wave_ref, atten_ref, sensor_ref, source_ref, other_ref,
    scale_ref, weight_ref, tail_ref, shapes_ref, mixed_ref, rows_ref, cols_ref, twice_ref, square_ref,
    whole_ref, spread_ref, sums_ref,
):
    modes = sensor_ref.shape[1]
    mine = grid_ref[0]
    first = mine == 0
    count = counts_ref[mine]

    wave = wave_ref[pl.ds(mine, 1), :]
    atten = atten_ref[pl.ds(mine, 1), :]
    ranges = 1.0 + lax.broadcasted_iota(jnp.int32, (RANGES, modes), 0).astype(jnp.float32)
    phase = wave * ranges
    keep = lax.broadcasted_iota(jnp.int32, (RANGES, modes), 1) < count
    magnitude = jnp.where(keep, jnp.exp(-atten * ranges) / jnp.sqrt(wave), 0.0)
    rows_ref[...] = jnp.zeros_like(rows_ref)
    for part, value in enumerate((magnitude * jnp.cos(phase), magnitude * jnp.sin(phase))):
        rows_ref[part, :RANGES, :modes] = value
        cols_ref[part] = rows_ref[part].T[:modes]
    spread_ref[...] = jnp.zeros_like(spread_ref)
    spread_ref[0, :, :modes] = jnp.broadcast_to(wave, (LANES, modes))
    spread_ref[1, :, :modes] = jnp.broadcast_to(atten, (LANES, modes))
    waves, attens = spread_ref[0], spread_ref[1]
    decay = jnp.exp(-(attens.T + attens))
    twice_ref[...] = (2.0 * decay * jnp.cos(waves - waves.T))[:modes]
    square_ref[...] = (decay * decay)[:modes]

    own_shape, other_shape = sensor_ref[mine], other_ref[0]
    own_depth, other_depth = source_ref[mine], other_ref[1]
    whole_ref[...] = jnp.zeros_like(whole_ref)
    whole_ref[:modes, :LANES] = jnp.where(first, own_shape, other_shape)
    whole_ref[:modes, LANES:] = jnp.where(first, other_shape, own_shape)
    shapes = whole_ref[...]
    sensors = shapes.shape[1]
    high, low = split(shapes)
    shapes_ref[:LANES] = high
    shapes_ref[LANES:] = low
    gram = (
        dot(high[:modes], high, ((1,), (1,)))
        + dot(low[:modes], high, ((1,), (1,)))
        + dot(high[:modes], low, ((1,), (1,)))
    )
    source = lax.broadcasted_iota(jnp.int32, (sensors, sensors), 0)
    target = lax.broadcasted_iota(jnp.int32, (sensors, sensors), 1)
    rows = sensors // 4
    order = (source == 4 * (target % rows) + target // rows).astype(jnp.bfloat16)
    mixed_ref[:modes] = dot(high[:modes], order).astype(jnp.bfloat16)
    mixed_ref[modes:] = dot(low[:modes], order).astype(jnp.bfloat16)
    depth = jnp.concatenate(
        [jnp.where(first, own_depth, other_depth), jnp.where(first, other_depth, own_depth)], 1
    )
    depth_high = depth.astype(jnp.bfloat16)
    tail_ref[...] = depth + (depth - depth_high.astype(jnp.float32))
    weight_ref[...] = jnp.zeros_like(weight_ref)
    weight_ref[:modes] = depth_high
    weight_ref[LANES : LANES + modes] = depth_high

    def exact(j):
        (left_real, left_imag), (right_real, right_imag) = pair(rows_ref, cols_ref, j)
        return gram * (left_real * right_real + left_imag * right_imag)

    total = forms(exact, twice_ref, square_ref, weight_ref, tail_ref, sums_ref)
    scale_ref[...] = 1.0 / (total * bins)


def numer_kernel(
    spectra_ref, scale_ref, weight_ref, tail_ref, shapes_ref, mixed_ref, rows_ref, cols_ref, twice_ref, square_ref,
    power_ref, whole_ref, real_ref, imag_ref, sums_ref,
):
    modes = tail_ref.shape[0]
    rows = spectra_ref.shape[0] // 8
    matrix = jnp.concatenate(
        [
            jnp.concatenate([spectra_ref[pl.ds(4 * half + k, rows, stride=8), :] for half in range(2)], 1)
            for k in range(4)
        ],
        0,
    )
    high, low = split(matrix)
    both = dot(mixed_ref[...], high)
    product = both[:modes] + both[modes:] + dot(mixed_ref[:modes], low)
    product_high, product_low = split(product)
    shape_high, shape_low = shapes_ref[:LANES], shapes_ref[LANES:]
    whole_ref[...] = jnp.zeros_like(whole_ref)
    whole_ref[:modes] = (
        dot(product_high, shape_high, ((1,), (1,)))
        + dot(product_low, shape_high, ((1,), (1,)))
        + dot(product_high, shape_low, ((1,), (1,)))
    )
    square = whole_ref[...]
    turned = square.T
    real_ref[...] = (0.5 * (square + turned))[:modes]
    imag_ref[...] = (0.5 * (square - turned))[:modes]

    def exact(j):
        (left_real, left_imag), (right_real, right_imag) = pair(rows_ref, cols_ref, j)
        even = left_real * right_real + left_imag * right_imag
        odd = left_real * right_imag - left_imag * right_real
        return real_ref[...] * even - imag_ref[...] * odd

    power = forms(exact, twice_ref, square_ref, weight_ref, tail_ref, sums_ref) * scale_ref[...]
    power_ref[pl.ds(0, RANGES, stride=2), :] = power[:, :LANES]
    power_ref[pl.ds(1, RANGES, stride=2), :] = power[:, LANES:]


def sum_kernel(parts_ref, total_ref):
    total_ref[...] = jnp.sum(parts_ref[...], 0, keepdims=True)


def shape_of(*shape, dtype=jnp.float32):
    return jax.ShapeDtypeStruct(shape, dtype)


def per_device(cross_spectra, sensor_modes, source_modes, wavenumber, attenuation, mode_counts):
    modes = sensor_modes.shape[1]
    sensors = cross_spectra.shape[3] * 2
    depths = source_modes.shape[2] * 2
    bins = cross_spectra.shape[1]
    mine = lax.axis_index("grid").astype(jnp.int32)
    where = mine.reshape(1)
    outgoing = pl.pallas_call(
        halves_kernel,
        out_shape=pltpu.VMEM((2, modes, LANES), jnp.float32),
        in_specs=[HBM, HBM],
        out_specs=VMEM,
        scratch_shapes=[pltpu.SemaphoreType.DMA((2,))],
        cost_estimate=COST,
        name="halves",
    )(sensor_modes, source_modes)
    incoming = lax.ppermute(outgoing, "grid", [(0, 1), (1, 0)])
    packed = pl.pallas_call(
        pack_kernel,
        out_shape=shape_of(bins * 4, LANES),
        in_specs=[VMEM],
        out_specs=VMEM,
        cost_estimate=COST,
        compiler_params=PARAMS,
        name="pack",
    )(cross_spectra.reshape(2, bins * 4, LANES))
    spectra = lax.all_to_all(packed.reshape(bins, 4, LANES), ("freq", "grid"), 0, 0, tiled=True)
    tables = pl.pallas_call(
        functools.partial(denom_kernel, bins),
        out_shape=[
            shape_of(RANGES, depths),
            shape_of(2 * LANES, depths, dtype=jnp.bfloat16),
            shape_of(modes, depths),
            shape_of(2 * LANES, sensors, dtype=jnp.bfloat16),
            shape_of(2 * modes, sensors, dtype=jnp.bfloat16),
            shape_of(2, LANES, LANES),
            shape_of(2, modes, LANES),
            shape_of(modes, LANES),
            shape_of(modes, LANES),
        ],
        in_specs=[SMEM, SMEM, VMEM, VMEM, VMEM, VMEM, VMEM],
        out_specs=[VMEM] * 9,
        scratch_shapes=[
            pltpu.VMEM((LANES, sensors), jnp.float32),
            pltpu.VMEM((2, LANES, LANES), jnp.float32),
            pltpu.VMEM((2, RANGES * 8, LANES), jnp.float32),
        ],
        cost_estimate=COST,
        compiler_params=PARAMS,
        name="denom",
    )(where, mode_counts, wavenumber, attenuation, sensor_modes, source_modes, incoming)
    power = pl.pallas_call(
        numer_kernel,
        out_shape=shape_of(RANGES * 2, LANES),
        in_specs=[VMEM] * 10,
        out_specs=VMEM,
        scratch_shapes=[
            pltpu.VMEM((LANES, LANES), jnp.float32),
            pltpu.VMEM((modes, LANES), jnp.float32),
            pltpu.VMEM((modes, LANES), jnp.float32),
            pltpu.VMEM((2, RANGES * 8, LANES), jnp.float32),
        ],
        cost_estimate=COST,
        compiler_params=PARAMS,
        name="numer",
    )(spectra.reshape(-1, LANES), *tables)
    parts = lax.all_to_all(power.reshape(-1, 1, LANES), ("freq", "grid"), 0, 0, tiled=True)
    return pl.pallas_call(
        sum_kernel,
        out_shape=shape_of(1, LANES),
        in_specs=[VMEM],
        out_specs=VMEM,
        compiler_params=PARAMS,
        name="total",
    )(parts.reshape(-1, LANES))


def solution(mesh):
    placed = (
        P(None, None, "freq", "grid"),
        P("freq", None, "grid"),
        P("freq", None, "grid"),
        P("freq", None),
        P("freq", None),
        P("freq"),
    )
    return jax.shard_map(
        per_device, mesh=mesh, in_specs=placed, out_specs=P("freq", "grid"), check_vma=False
    )
```

```python
import functools

import jax
import jax.numpy as jnp
from jax import lax
from jax.experimental import pallas as pl
from jax.experimental.pallas import tpu as pltpu
from jax.sharding import PartitionSpec as P


RANGES = 64
LANES = 128
CHUNK = 32

VMEM = pl.BlockSpec(memory_space=pltpu.VMEM)
HBM = pl.BlockSpec(memory_space=pltpu.HBM)
SMEM = pl.BlockSpec(memory_space=pltpu.SMEM)
COST = pl.CostEstimate(flops=8_000_000_000, bytes_accessed=0, transcendentals=0)
PARAMS = pltpu.CompilerParams(vmem_limit_bytes=8 * 1024 * 1024)


def split(value):
    high = value.astype(jnp.bfloat16)
    low = (value - high.astype(jnp.float32)).astype(jnp.bfloat16)
    return high, low


def dot(left, right, contract=((1,), (0,))):
    return lax.dot_general(left, right, (contract, ((), ())), preferred_element_type=jnp.float32)


def halves_kernel(sensor_ref, source_ref, outgoing_ref, sem):
    other = 1 - lax.axis_index("grid")
    copies = [
        pltpu.make_async_copy(ref.at[other], outgoing_ref.at[k], sem.at[k])
        for k, ref in enumerate((sensor_ref, source_ref))
    ]
    for copy in copies:
        copy.start()
    for copy in copies:
        copy.wait()


def pack_kernel(spectra_ref, packed_ref):
    packed_ref[...] = spectra_ref[0] + spectra_ref[1]


def forms(exact, twice_ref, square_ref, weight, tail, sums_ref):
    modes = tail.shape[0]
    depths = tail.shape[1]
    for base in range(0, RANGES, CHUNK):
        left = []
        before = now = None
        for j in range(base, base + CHUNK):
            if j < base + 2:
                later = exact(j)
            else:
                later = twice_ref[...] * now - square_ref[...] * before
            before, now = now, later
            high, low = split(now)
            left.append(jnp.concatenate([high, low], 1))
        image = dot(jnp.concatenate(left, 0), weight[...])
        for k in range(CHUNK):
            terms = tail[...] * image[k * modes : (k + 1) * modes]
            sums = jnp.sum(terms.reshape(-1, 8, depths), 0)
            row = (base + k) * 8
            for half in range(2):
                sums_ref[half, row : row + 8, :] = sums[:, half * LANES : (half + 1) * LANES]
    totals = []
    for half in range(2):
        total = sums_ref[half, pl.ds(0, RANGES, stride=8), :]
        for k in range(1, 8):
            total = total + sums_ref[half, pl.ds(k, RANGES, stride=8), :]
        totals.append(total)
    return jnp.concatenate(totals, 1)


def pair(rows_ref, cols_ref, j):
    modes = cols_ref.shape[1]
    left = [jnp.broadcast_to(cols_ref[part, :, j : j + 1], (modes, LANES)) for part in range(2)]
    right = [rows_ref[part, j : j + 1, :] for part in range(2)]
    return left, right


def denom_kernel(
    bins, grid_ref, counts_ref, wave_ref, atten_ref, sensor_ref, source_ref, other_ref,
    scale_ref, weight_ref, tail_ref, shapes_ref, mixed_ref, rows_ref, cols_ref, twice_ref, square_ref,
    whole_ref, spread_ref, sums_ref,
):
    modes = sensor_ref.shape[1]
    mine = grid_ref[0]
    first = mine == 0
    count = counts_ref[mine]

    wave = wave_ref[pl.ds(mine, 1), :]
    atten = atten_ref[pl.ds(mine, 1), :]
    ranges = 1.0 + lax.broadcasted_iota(jnp.int32, (RANGES, modes), 0).astype(jnp.float32)
    phase = wave * ranges
    keep = lax.broadcasted_iota(jnp.int32, (RANGES, modes), 1) < count
    magnitude = jnp.where(keep, jnp.exp(-atten * ranges) / jnp.sqrt(wave), 0.0)
    rows_ref[...] = jnp.zeros_like(rows_ref)
    for part, value in enumerate((magnitude * jnp.cos(phase), magnitude * jnp.sin(phase))):
        rows_ref[part, :RANGES, :modes] = value
        cols_ref[part] = rows_ref[part].T[:modes]
    spread_ref[...] = jnp.zeros_like(spread_ref)
    spread_ref[0, :, :modes] = jnp.broadcast_to(wave, (LANES, modes))
    spread_ref[1, :, :modes] = jnp.broadcast_to(atten, (LANES, modes))
    waves, attens = spread_ref[0], spread_ref[1]
    decay = jnp.exp(-(attens.T + attens))
    twice_ref[...] = (2.0 * decay * jnp.cos(waves - waves.T))[:modes]
    square_ref[...] = (decay * decay)[:modes]

    own_shape, other_shape = sensor_ref[mine], other_ref[0]
    own_depth, other_depth = source_ref[mine], other_ref[1]
    whole_ref[...] = jnp.zeros_like(whole_ref)
    whole_ref[:modes, :LANES] = jnp.where(first, own_shape, other_shape)
    whole_ref[:modes, LANES:] = jnp.where(first, other_shape, own_shape)
    shapes = whole_ref[...]
    sensors = shapes.shape[1]
    high, low = split(shapes)
    shapes_ref[:LANES] = high
    shapes_ref[LANES:] = low
    gram = (
        dot(high[:modes], high, ((1,), (1,)))
        + dot(low[:modes], high, ((1,), (1,)))
        + dot(high[:modes], low, ((1,), (1,)))
    )
    source = lax.broadcasted_iota(jnp.int32, (sensors, sensors), 0)
    target = lax.broadcasted_iota(jnp.int32, (sensors, sensors), 1)
    rows = sensors // 4
    order = (source == 4 * (target % rows) + target // rows).astype(jnp.bfloat16)
    mixed_ref[:modes] = dot(high[:modes], order).astype(jnp.bfloat16)
    mixed_ref[modes:] = dot(low[:modes], order).astype(jnp.bfloat16)
    depth = jnp.concatenate(
        [jnp.where(first, own_depth, other_depth), jnp.where(first, other_depth, own_depth)], 1
    )
    depth_high = depth.astype(jnp.bfloat16)
    tail_ref[...] = depth + (depth - depth_high.astype(jnp.float32))
    weight_ref[...] = jnp.zeros_like(weight_ref)
    weight_ref[:modes] = depth_high
    weight_ref[LANES : LANES + modes] = depth_high

    def exact(j):
        (left_real, left_imag), (right_real, right_imag) = pair(rows_ref, cols_ref, j)
        return gram * (left_real * right_real + left_imag * right_imag)

    total = forms(exact, twice_ref, square_ref, weight_ref, tail_ref, sums_ref)
    scale_ref[...] = 1.0 / (total * bins)


def numer_kernel(
    spectra_ref, scale_ref, weight_ref, tail_ref, shapes_ref, mixed_ref, rows_ref, cols_ref, twice_ref, square_ref,
    power_ref, whole_ref, real_ref, imag_ref, sums_ref,
):
    modes = tail_ref.shape[0]
    rows = spectra_ref.shape[0] // 8
    matrix = jnp.concatenate(
        [
            jnp.concatenate([spectra_ref[pl.ds(4 * half + k, rows, stride=8), :] for half in range(2)], 1)
            for k in range(4)
        ],
        0,
    )
    high, low = split(matrix)
    both = dot(mixed_ref[...], high)
    rest = dot(mixed_ref[:modes], low)
    product = both[:modes] + (both[modes:] + rest)
    product_high, product_low = split(product)
    shape_high, shape_low = shapes_ref[:LANES], shapes_ref[LANES:]
    whole_ref[...] = jnp.zeros_like(whole_ref)
    sums = dot(jnp.concatenate([product_high, product_low], 0), shape_high, ((1,), (1,)))
    whole_ref[:modes] = sums[:modes] + sums[modes:] + dot(product_high, shape_low, ((1,), (1,)))
    square = whole_ref[...]
    turned = square.T
    real_ref[...] = (0.5 * (square + turned))[:modes]
    imag_ref[...] = (0.5 * (square - turned))[:modes]

    def exact(j):
        (left_real, left_imag), (right_real, right_imag) = pair(rows_ref, cols_ref, j)
        even = left_real * right_real + left_imag * right_imag
        odd = left_real * right_imag - left_imag * right_real
        return real_ref[...] * even - imag_ref[...] * odd

    power = forms(exact, twice_ref, square_ref, weight_ref, tail_ref, sums_ref) * scale_ref[...]
    power_ref[pl.ds(0, RANGES, stride=2), :] = power[:, :LANES]
    power_ref[pl.ds(1, RANGES, stride=2), :] = power[:, LANES:]


def sum_kernel(parts_ref, total_ref):
    total_ref[...] = jnp.sum(parts_ref[...], 0, keepdims=True)


def shape_of(*shape, dtype=jnp.float32):
    return jax.ShapeDtypeStruct(shape, dtype)


def per_device(cross_spectra, sensor_modes, source_modes, wavenumber, attenuation, mode_counts):
    modes = sensor_modes.shape[1]
    sensors = cross_spectra.shape[3] * 2
    depths = source_modes.shape[2] * 2
    bins = cross_spectra.shape[1]
    mine = lax.axis_index("grid").astype(jnp.int32)
    where = mine.reshape(1)
    outgoing = pl.pallas_call(
        halves_kernel,
        out_shape=pltpu.VMEM((2, modes, LANES), jnp.float32),
        in_specs=[HBM, HBM],
        out_specs=VMEM,
        scratch_shapes=[pltpu.SemaphoreType.DMA((2,))],
        cost_estimate=COST,
        name="halves",
    )(sensor_modes, source_modes)
    incoming = lax.ppermute(outgoing, "grid", [(0, 1), (1, 0)])
    packed = pl.pallas_call(
        pack_kernel,
        out_shape=shape_of(bins * 4, LANES),
        in_specs=[VMEM],
        out_specs=VMEM,
        cost_estimate=COST,
        compiler_params=PARAMS,
        name="pack",
    )(cross_spectra.reshape(2, bins * 4, LANES))
    spectra = lax.all_to_all(packed.reshape(bins, 4, LANES), ("freq", "grid"), 0, 0, tiled=True)
    tables = pl.pallas_call(
        functools.partial(denom_kernel, bins),
        out_shape=[
            shape_of(RANGES, depths),
            shape_of(2 * LANES, depths, dtype=jnp.bfloat16),
            shape_of(modes, depths),
            shape_of(2 * LANES, sensors, dtype=jnp.bfloat16),
            shape_of(2 * modes, sensors, dtype=jnp.bfloat16),
            shape_of(2, LANES, LANES),
            shape_of(2, modes, LANES),
            shape_of(modes, LANES),
            shape_of(modes, LANES),
        ],
        in_specs=[SMEM, SMEM, VMEM, VMEM, VMEM, VMEM, VMEM],
        out_specs=[VMEM] * 9,
        scratch_shapes=[
            pltpu.VMEM((LANES, sensors), jnp.float32),
            pltpu.VMEM((2, LANES, LANES), jnp.float32),
            pltpu.VMEM((2, RANGES * 8, LANES), jnp.float32),
        ],
        cost_estimate=COST,
        compiler_params=PARAMS,
        name="denom",
    )(where, mode_counts, wavenumber, attenuation, sensor_modes, source_modes, incoming)
    power = pl.pallas_call(
        numer_kernel,
        out_shape=shape_of(RANGES * 2, LANES),
        in_specs=[VMEM] * 10,
        out_specs=VMEM,
        scratch_shapes=[
            pltpu.VMEM((LANES, LANES), jnp.float32),
            pltpu.VMEM((modes, LANES), jnp.float32),
            pltpu.VMEM((modes, LANES), jnp.float32),
            pltpu.VMEM((2, RANGES * 8, LANES), jnp.float32),
        ],
        cost_estimate=COST,
        compiler_params=PARAMS,
        name="numer",
    )(spectra.reshape(-1, LANES), *tables)
    parts = lax.all_to_all(power.reshape(-1, 1, LANES), ("freq", "grid"), 0, 0, tiled=True)
    return pl.pallas_call(
        sum_kernel,
        out_shape=shape_of(1, LANES),
        in_specs=[VMEM],
        out_specs=VMEM,
        compiler_params=PARAMS,
        name="total",
    )(parts.reshape(-1, LANES))


def solution(mesh):
    placed = (
        P(None, None, "freq", "grid"),
        P("freq", None, "grid"),
        P("freq", None, "grid"),
        P("freq", None),
        P("freq", None),
        P("freq"),
    )
    return jax.shard_map(
        per_device, mesh=mesh, in_specs=placed, out_specs=P("freq", "grid"), check_vma=False
    )
```

```python
import functools

import jax
import jax.numpy as jnp
from jax import lax
from jax.experimental import pallas as pl
from jax.experimental.pallas import tpu as pltpu
from jax.sharding import PartitionSpec as P


RANGES = 64
LANES = 128
CHUNK = 32
GROUP = 16

VMEM = pl.BlockSpec(memory_space=pltpu.VMEM)
HBM = pl.BlockSpec(memory_space=pltpu.HBM)
SMEM = pl.BlockSpec(memory_space=pltpu.SMEM)
COST = pl.CostEstimate(flops=8_000_000_000, bytes_accessed=0, transcendentals=0)
PARAMS = pltpu.CompilerParams(vmem_limit_bytes=8 * 1024 * 1024)


def split(value):
    high = value.astype(jnp.bfloat16)
    low = (value - high.astype(jnp.float32)).astype(jnp.bfloat16)
    return high, low


def dot(left, right, contract=((1,), (0,))):
    return lax.dot_general(left, right, (contract, ((), ())), preferred_element_type=jnp.float32)


def halves_kernel(sensor_ref, source_ref, outgoing_ref, sem):
    other = 1 - lax.axis_index("grid")
    copies = [
        pltpu.make_async_copy(ref.at[other], outgoing_ref.at[k], sem.at[k])
        for k, ref in enumerate((sensor_ref, source_ref))
    ]
    for copy in copies:
        copy.start()
    for copy in copies:
        copy.wait()


def pack_kernel(spectra_ref, packed_ref):
    packed_ref[...] = spectra_ref[0] + spectra_ref[1]


def forms(exact, twice_ref, square_ref, weight, tail, sums_ref):
    modes = tail.shape[0]
    depths = tail.shape[1]
    before = now = None
    for base in range(0, RANGES, GROUP):
        left = []
        for j in range(base, base + GROUP):
            if j % CHUNK < 2:
                later = exact(j)
            else:
                later = twice_ref[...] * now - square_ref[...] * before
            before, now = now, later
            high, low = split(now)
            left.append(jnp.concatenate([high, low], 1))
        image = dot(jnp.concatenate(left, 0), weight[...])
        for k in range(GROUP):
            terms = tail[...] * image[k * modes : (k + 1) * modes]
            sums = jnp.sum(terms.reshape(-1, 8, depths), 0)
            row = (base + k) * 8
            for half in range(2):
                sums_ref[half, row : row + 8, :] = sums[:, half * LANES : (half + 1) * LANES]
    totals = []
    for half in range(2):
        total = sums_ref[half, pl.ds(0, RANGES, stride=8), :]
        for k in range(1, 8):
            total = total + sums_ref[half, pl.ds(k, RANGES, stride=8), :]
        totals.append(total)
    return jnp.concatenate(totals, 1)


def pair(rows_ref, cols_ref, j):
    modes = cols_ref.shape[1]
    left = [jnp.broadcast_to(cols_ref[part, :, j : j + 1], (modes, LANES)) for part in range(2)]
    right = [rows_ref[part, j : j + 1, :] for part in range(2)]
    return left, right


def denom_kernel(
    bins, grid_ref, counts_ref, wave_ref, atten_ref, sensor_ref, source_ref, other_ref,
    scale_ref, weight_ref, tail_ref, shapes_ref, mixed_ref, rows_ref, cols_ref, twice_ref, square_ref,
    whole_ref, spread_ref, sums_ref,
):
    modes = sensor_ref.shape[1]
    mine = grid_ref[0]
    first = mine == 0
    count = counts_ref[mine]

    wave = wave_ref[pl.ds(mine, 1), :]
    atten = atten_ref[pl.ds(mine, 1), :]
    ranges = 1.0 + lax.broadcasted_iota(jnp.int32, (RANGES, modes), 0).astype(jnp.float32)
    phase = wave * ranges
    keep = lax.broadcasted_iota(jnp.int32, (RANGES, modes), 1) < count
    magnitude = jnp.where(keep, jnp.exp(-atten * ranges) / jnp.sqrt(wave), 0.0)
    rows_ref[...] = jnp.zeros_like(rows_ref)
    for part, value in enumerate((magnitude * jnp.cos(phase), magnitude * jnp.sin(phase))):
        rows_ref[part, :RANGES, :modes] = value
        cols_ref[part] = rows_ref[part].T[:modes]
    spread_ref[...] = jnp.zeros_like(spread_ref)
    spread_ref[0, :, :modes] = jnp.broadcast_to(wave, (LANES, modes))
    spread_ref[1, :, :modes] = jnp.broadcast_to(atten, (LANES, modes))
    waves, attens = spread_ref[0], spread_ref[1]
    decay = jnp.exp(-(attens.T + attens))
    twice_ref[...] = (2.0 * decay * jnp.cos(waves - waves.T))[:modes]
    square_ref[...] = (decay * decay)[:modes]

    own_shape, other_shape = sensor_ref[mine], other_ref[0]
    own_depth, other_depth = source_ref[mine], other_ref[1]
    whole_ref[...] = jnp.zeros_like(whole_ref)
    whole_ref[:modes, :LANES] = jnp.where(first, own_shape, other_shape)
    whole_ref[:modes, LANES:] = jnp.where(first, other_shape, own_shape)
    shapes = whole_ref[...]
    sensors = shapes.shape[1]
    high, low = split(shapes)
    shapes_ref[:LANES] = high
    shapes_ref[LANES:] = low
    gram = (
        dot(high[:modes], high, ((1,), (1,)))
        + dot(low[:modes], high, ((1,), (1,)))
        + dot(high[:modes], low, ((1,), (1,)))
    )
    source = lax.broadcasted_iota(jnp.int32, (sensors, sensors), 0)
    target = lax.broadcasted_iota(jnp.int32, (sensors, sensors), 1)
    rows = sensors // 4
    order = (source == 4 * (target % rows) + target // rows).astype(jnp.bfloat16)
    mixed_ref[:modes] = dot(high[:modes], order).astype(jnp.bfloat16)
    mixed_ref[modes:] = dot(low[:modes], order).astype(jnp.bfloat16)
    depth = jnp.concatenate(
        [jnp.where(first, own_depth, other_depth), jnp.where(first, other_depth, own_depth)], 1
    )
    depth_high = depth.astype(jnp.bfloat16)
    tail_ref[...] = depth + (depth - depth_high.astype(jnp.float32))
    weight_ref[...] = jnp.zeros_like(weight_ref)
    weight_ref[:modes] = depth_high
    weight_ref[LANES : LANES + modes] = depth_high

    def exact(j):
        (left_real, left_imag), (right_real, right_imag) = pair(rows_ref, cols_ref, j)
        return gram * (left_real * right_real + left_imag * right_imag)

    total = forms(exact, twice_ref, square_ref, weight_ref, tail_ref, sums_ref)
    scale_ref[...] = 1.0 / (total * bins)


def numer_kernel(
    spectra_ref, scale_ref, weight_ref, tail_ref, shapes_ref, mixed_ref, rows_ref, cols_ref, twice_ref, square_ref,
    power_ref, whole_ref, real_ref, imag_ref, sums_ref,
):
    modes = tail_ref.shape[0]
    rows = spectra_ref.shape[0] // 8
    matrix = jnp.concatenate(
        [
            jnp.concatenate([spectra_ref[pl.ds(4 * half + k, rows, stride=8), :] for half in range(2)], 1)
            for k in range(4)
        ],
        0,
    )
    high, low = split(matrix)
    both = dot(mixed_ref[...], high)
    product = both[:modes] + both[modes:] + dot(mixed_ref[:modes], low)
    product_high, product_low = split(product)
    shape_high, shape_low = shapes_ref[:LANES], shapes_ref[LANES:]
    whole_ref[...] = jnp.zeros_like(whole_ref)
    whole_ref[:modes] = (
        dot(product_high, shape_high, ((1,), (1,)))
        + dot(product_low, shape_high, ((1,), (1,)))
        + dot(product_high, shape_low, ((1,), (1,)))
    )
    square = whole_ref[...]
    turned = square.T
    real_ref[...] = (0.5 * (square + turned))[:modes]
    imag_ref[...] = (0.5 * (square - turned))[:modes]

    def exact(j):
        (left_real, left_imag), (right_real, right_imag) = pair(rows_ref, cols_ref, j)
        even = left_real * right_real + left_imag * right_imag
        odd = left_real * right_imag - left_imag * right_real
        return real_ref[...] * even - imag_ref[...] * odd

    power = forms(exact, twice_ref, square_ref, weight_ref, tail_ref, sums_ref) * scale_ref[...]
    power_ref[pl.ds(0, RANGES, stride=2), :] = power[:, :LANES]
    power_ref[pl.ds(1, RANGES, stride=2), :] = power[:, LANES:]


def sum_kernel(parts_ref, total_ref):
    total_ref[...] = jnp.sum(parts_ref[...], 0, keepdims=True)


def shape_of(*shape, dtype=jnp.float32):
    return jax.ShapeDtypeStruct(shape, dtype)


def per_device(cross_spectra, sensor_modes, source_modes, wavenumber, attenuation, mode_counts):
    modes = sensor_modes.shape[1]
    sensors = cross_spectra.shape[3] * 2
    depths = source_modes.shape[2] * 2
    bins = cross_spectra.shape[1]
    mine = lax.axis_index("grid").astype(jnp.int32)
    where = mine.reshape(1)
    outgoing = pl.pallas_call(
        halves_kernel,
        out_shape=pltpu.VMEM((2, modes, LANES), jnp.float32),
        in_specs=[HBM, HBM],
        out_specs=VMEM,
        scratch_shapes=[pltpu.SemaphoreType.DMA((2,))],
        cost_estimate=COST,
        name="halves",
    )(sensor_modes, source_modes)
    incoming = lax.ppermute(outgoing, "grid", [(0, 1), (1, 0)])
    packed = pl.pallas_call(
        pack_kernel,
        out_shape=shape_of(bins * 4, LANES),
        in_specs=[VMEM],
        out_specs=VMEM,
        cost_estimate=COST,
        compiler_params=PARAMS,
        name="pack",
    )(cross_spectra.reshape(2, bins * 4, LANES))
    spectra = lax.all_to_all(packed.reshape(bins, 4, LANES), ("freq", "grid"), 0, 0, tiled=True)
    tables = pl.pallas_call(
        functools.partial(denom_kernel, bins),
        out_shape=[
            shape_of(RANGES, depths),
            shape_of(2 * LANES, depths, dtype=jnp.bfloat16),
            shape_of(modes, depths),
            shape_of(2 * LANES, sensors, dtype=jnp.bfloat16),
            shape_of(2 * modes, sensors, dtype=jnp.bfloat16),
            shape_of(2, LANES, LANES),
            shape_of(2, modes, LANES),
            shape_of(modes, LANES),
            shape_of(modes, LANES),
        ],
        in_specs=[SMEM, SMEM, VMEM, VMEM, VMEM, VMEM, VMEM],
        out_specs=[VMEM] * 9,
        scratch_shapes=[
            pltpu.VMEM((LANES, sensors), jnp.float32),
            pltpu.VMEM((2, LANES, LANES), jnp.float32),
            pltpu.VMEM((2, RANGES * 8, LANES), jnp.float32),
        ],
        cost_estimate=COST,
        compiler_params=PARAMS,
        name="denom",
    )(where, mode_counts, wavenumber, attenuation, sensor_modes, source_modes, incoming)
    power = pl.pallas_call(
        numer_kernel,
        out_shape=shape_of(RANGES * 2, LANES),
        in_specs=[VMEM] * 10,
        out_specs=VMEM,
        scratch_shapes=[
            pltpu.VMEM((LANES, LANES), jnp.float32),
            pltpu.VMEM((modes, LANES), jnp.float32),
            pltpu.VMEM((modes, LANES), jnp.float32),
            pltpu.VMEM((2, RANGES * 8, LANES), jnp.float32),
        ],
        cost_estimate=COST,
        compiler_params=PARAMS,
        name="numer",
    )(spectra.reshape(-1, LANES), *tables)
    parts = lax.all_to_all(power.reshape(-1, 1, LANES), ("freq", "grid"), 0, 0, tiled=True)
    return pl.pallas_call(
        sum_kernel,
        out_shape=shape_of(1, LANES),
        in_specs=[VMEM],
        out_specs=VMEM,
        compiler_params=PARAMS,
        name="total",
    )(parts.reshape(-1, LANES))


def solution(mesh):
    placed = (
        P(None, None, "freq", "grid"),
        P("freq", None, "grid"),
        P("freq", None, "grid"),
        P("freq", None),
        P("freq", None),
        P("freq"),
    )
    return jax.shard_map(
        per_device, mesh=mesh, in_specs=placed, out_specs=P("freq", "grid"), check_vma=False
    )
```
